256 devices in a mesh: mom: 16 (over x, y_hi, core), col: 16 (over z, y_lo).
Axes of the slice: x: 4, y: 4 (y_hi: 2, y_lo: 2; y = y_hi * 2 + y_lo), z: 8, core: 2. Of those that a mesh axis runs over, the one named last changes fastest.
Arguments:
- vertex: bfloat16 [32768, 32768], P('mom', 'col'), may hold values from -1 to 1, as said below
- sources: bfloat16 [128, 32768], P('col', 'mom'), may hold values from -6 to 6
- green_fn: float32 [32768], P('mom'), may hold values from -1.2 to 1.2
- green_shifted: float32 [32768], P('mom'), may hold values from -1.2 to 1.2
- leg_weights: float32 [128], P('col'), may hold values from -0.25 to 0.25
Outputs:
- ladder: float32 [128, 32768], P('col', 'mom')
- dressed: float32 [32768], P('mom')
The draws below stay inside these ranges and needn't reach their ends.
Inputs may be any that keep to these rules, and one draw needn't show every extreme that they name: vertex equals its own transpose.
All inputs are finite; a program needn't handle non-finite values.
Results may differ from the reference program's by a relative error of at most 0.0023.
Values may be sent and summed in bfloat16 or wider, within the bound.
A program may use at most 64 MiB of HBM per device.

```python
import math
import jax
import jax.numpy as jnp
from jax import lax

K = 16
P_SIZE = 8
NF = 256
M = 32768
R = 128
SWEEPS = 3


def draw_vertex(key, part):
    block_size = math.gcd(M, 512)
    block_count = M // block_size
    factor = 1.5 / math.sqrt(M)

    def row_block(row_index):

        def single_tile(col_index):
            lower = jnp.minimum(row_index, col_index)
            upper = jnp.maximum(row_index, col_index)
            tile_key = jax.random.fold_in(key, lower * block_count + upper)
            values = jnp.clip(jax.random.normal(tile_key, (block_size, block_size), jnp.float32), -6.0, 6.0)
            mirrored = jnp.where(row_index < col_index, values, values.T)
            return jnp.where(row_index == col_index, (values + values.T) * 0.5, mirrored)
        tiles = lax.map(single_tile, jnp.arange(block_count))
        joined = jnp.transpose(tiles, (1, 0, 2)).reshape(block_size, M)
        return (joined * factor).astype(jnp.bfloat16)
    blocks = lax.map(row_block, jnp.arange(block_count))
    return blocks.reshape(M, M)


def drawn_green(key, salt):
    base_key = jax.random.fold_in(key, salt)
    return jax.random.uniform(base_key, (M,), jnp.float32, -1.2, 1.2)


def draw_green_fn(key, part):
    return drawn_green(key, 7101)


def draw_green_shifted(key, part):
    return drawn_green(key, 7202)


def level_of(key, shape, cuts, least, high):
    gain, own = 1.0, jax.random.fold_in(key, 6)
    for position, shards_of in cuts:
        heights = jnp.exp(jax.random.uniform(jax.random.fold_in(own, position), (shards_of,), jnp.float32, least / len(cuts), high / len(cuts)))
        gain = gain * jnp.repeat(heights, shape[position] // shards_of).reshape([-1 if axis == position else 1 for axis in range(len(shape))])
    return gain


def gaussian(rng, extent, scale, reach, pieces=(), dtype=jnp.bfloat16):
    array = scale * jax.random.normal(rng, extent, jnp.float32)
    if pieces:
        array = array * level_of(rng, extent, pieces, -0.22, 0.18)
    return jnp.clip(array, -reach, reach).astype(dtype)


def setup_inputs(seed: int = 0) -> dict:
    seeds = jax.random.split(jax.random.key(seed), 6)
    return {
        "vertex": draw_vertex(jax.random.fold_in(seeds[5], 71), 0),
        "sources": gaussian(seeds[1], (R, M), 1.0, 6.0, ((0, 16), (1, 16))),
        "green_fn": draw_green_fn(jax.random.fold_in(seeds[5], 71), 0),
        "green_shifted": draw_green_shifted(jax.random.fold_in(seeds[5], 71), 0),
        "leg_weights": gaussian(seeds[4], (R,), (4 * R) ** -0.5, 0.25, ((0, 16),), jnp.float32),
    }


def bubble_of(dressed_fn, shift_grid, slab_rows):
    grid_now = dressed_fn.reshape(K, slab_rows)
    ahead_slab = jnp.roll(shift_grid, -(K // 4), axis=0)
    behind_slab = jnp.roll(grid_now, K // 4, axis=0)
    return (-0.5 * (grid_now * ahead_slab + shift_grid * behind_slab)).reshape(M)


def reference(vertex, sources, green_fn, green_shifted, leg_weights):
    slab_rows = P_SIZE * NF
    shift_grid = green_shifted.reshape(K, slab_rows)
    source_wide = sources.astype(jnp.float32)

    def richardson_step(ladder_state, bubble_row):
        operand = ladder_state.astype(jnp.bfloat16)
        product = lax.dot_general(operand, vertex, (((1,), (1,)), ((), ())), preferred_element_type=jnp.float32)
        return bubble_row[None, :] * (source_wide + product)

    bubble_first = bubble_of(green_fn, shift_grid, slab_rows)
    ladder_state = bubble_first[None, :] * source_wide
    for sweep_index in range(SWEEPS):
        ladder_state = richardson_step(ladder_state, bubble_first)
    self_energy = jnp.dot(leg_weights, ladder_state, precision=lax.Precision.HIGHEST)
    dressed = green_fn + green_fn * green_fn * self_energy
    bubble_second = bubble_of(dressed, shift_grid, slab_rows)
    for sweep_index in range(SWEEPS):
        ladder_state = richardson_step(ladder_state, bubble_second)
    return ladder_state, dressed
```

```python
import functools

import jax
import jax.numpy as jnp
from jax import lax
from jax.experimental import pallas as pl
from jax.experimental.pallas import tpu as pltpu
from jax.sharding import PartitionSpec as P

MESH = pl.DeviceIdType.MESH
LANES = 128
ROWS = 8
F32 = jnp.float32
BF16 = jnp.bfloat16


class Axis:
    def __init__(self, name, which, size):
        self.name = name
        self.which = which
        self.size = size
        self.groups = size // 2
        self.me = lax.axis_index(name)
        self.parity = self.me % 2
        self.group = self.me // 2
        self.pair = self.me + 1 - 2 * self.parity

    def at(self, index):
        return {self.name: index}

    def mate(self, steps):
        return 2 * ((self.group + steps) % self.groups) + self.parity

    def order(self, k):
        sign = 2 * (k % 2) - 1
        return (self.groups // 2 + sign * ((k + 1) // 2) + self.groups) % self.groups


def remote(src, dst, send, recv, device):
    return pltpu.make_async_remote_copy(
        src_ref=src,
        dst_ref=dst,
        send_sem=send,
        recv_sem=recv,
        device_id=device,
        device_id_type=MESH,
    )


def loop(count, step):
    def run(k, carry):
        step(k)
        return carry

    lax.fori_loop(0, count, run, 0)


class Gather:
    def __init__(self, axis, buf, own, sems):
        self.axis, self.buf, self.own = axis, buf, own
        self.mate_send, self.mate_recv, self.pair_send, self.pair_recv = sems

    def mate_copy(self, t):
        a = self.axis
        return remote(
            self.own, self.buf.at[a.me], self.mate_send.at[t], self.mate_recv.at[t], a.at(a.mate(t))
        )

    def pair_copy(self, t, src):
        a = self.axis
        block = a.mate(a.groups - t)
        return remote(
            src, self.buf.at[block], self.pair_send.at[t], self.pair_recv.at[t], a.at(a.pair)
        )

    def start(self):
        a = self.axis
        self.pair_copy(0, self.own).start()
        loop(a.groups - 1, lambda k: self.mate_copy(a.order(k)).start())

    def forward(self, k):
        a = self.axis
        t = a.order(k)
        block = a.mate(a.groups - t)
        self.mate_copy(t).wait_recv()
        self.pair_copy(t, self.buf.at[block]).start()

    def forward_all(self):
        loop(self.axis.groups - 1, self.forward)

    def finish(self):
        a = self.axis

        def ended(k):
            t = a.order(k)
            copy = self.pair_copy(t, self.buf.at[a.me])
            copy.wait_recv()
            copy.wait_send()

        def sent(k):
            self.mate_copy(a.order(k)).wait_send()

        loop(a.groups, ended)
        loop(a.groups - 1, sent)


def kernel(
    size,
    ahead,
    v_hbm,
    src,
    g_in,
    s_in,
    w_in,
    lad_out,
    dre_out,
    v_mat,
    v_turned,
    x_mom,
    x_col,
    sbuf,
    wbuf,
    dvbuf,
    keep,
    give,
    taken,
    hand,
    landed,
    own,
    fin_wide,
    fin,
    fin_taken,
    fin_hand,
    fin_landed,
    b_full,
    s_ahead,
    g_behind,
    src_col,
    src_col_sent,
    src_mom,
    vec_sent,
    vec_mom,
    dre_sent,
    dre_behind,
    dv_sent,
    v_sem,
    shift_send,
    shift_recv,
    turn_send,
    turn_recv,
    behind_send,
    behind_recv,
    ag_sems,
    w_sems,
    dv_sems,
    rp_send,
    rp_recv,
    rg_send,
    rg_recv,
):
    mom = Axis("mom", 0, size)
    col = Axis("col", 1, size)
    groups = size // 2
    sources = size * ROWS
    block = size * LANES
    panel = 2 * LANES

    def v_copy(k):
        rows = pl.ds(pl.multiple_of(k * panel, panel), panel)
        return pltpu.make_async_copy(v_hbm.at[rows], v_mat.at[rows], v_sem.at[k])

    loop(groups, lambda k: v_copy(k).start())

    barrier = pltpu.get_barrier_semaphore()
    for a in (mom, col):
        pl.semaphore_signal(barrier, inc=1, device_id=a.at(a.pair), device_id_type=MESH)

        def greet(k, a=a):
            pl.semaphore_signal(barrier, inc=1, device_id=a.at(a.mate(k + 1)), device_id_type=MESH)

        loop(groups - 1, greet)
    turned = {"mom": col.me, "col": mom.me}
    off_diagonal = mom.me != col.me

    @pl.when(off_diagonal)
    def _():
        pl.semaphore_signal(barrier, inc=1, device_id=turned, device_id_type=MESH)

    @pl.when(off_diagonal)
    def _():
        pl.semaphore_wait(barrier, size + 1)

    @pl.when(jnp.logical_not(off_diagonal))
    def _():
        pl.semaphore_wait(barrier, size)

    def sems_of(ref, which):
        return tuple(ref.at[which, n] for n in range(4))

    to_behind = remote(
        s_in, s_ahead, shift_send.at[0], shift_recv.at[0], mom.at((mom.me + size - ahead) % size)
    )
    to_ahead = remote(g_in, g_behind, shift_send.at[1], shift_recv.at[1], mom.at((mom.me + ahead) % size))
    to_behind.start()
    to_ahead.start()
    source_gather = Gather(col, sbuf, src, sems_of(ag_sems, 1))
    source_gather.start()
    weight_gather = Gather(col, wbuf, w_in, sems_of(w_sems, 0))
    weight_gather.start()
    sbuf[col.me] = src[...]
    wbuf[col.me] = w_in[...]

    def turn_panel(k):
        v_copy(k).wait()
        rows = pl.ds(pl.multiple_of(k * panel, panel), panel)
        for n in range(groups):
            cols = slice(n * panel, (n + 1) * panel)
            v_turned[cols, rows] = v_mat[rows, cols].T

    def forward_and_turn(k):
        source_gather.forward(k)
        turn_panel(k)

    loop(groups - 1, forward_and_turn)
    turn_panel(groups - 1)
    weight_gather.forward_all()

    to_behind.wait()
    to_ahead.wait()
    b_full[...] = -0.5 * (g_in[...] * s_ahead[...] + s_in[...] * g_behind[...])
    source_gather.finish()

    def first_operand(k):
        two = sbuf[pl.ds(2 * k, 2)].astype(F32)
        rows = pl.ds(pl.multiple_of(2 * ROWS * k, 2 * ROWS), 2 * ROWS)
        for n in range(size):
            part = two[:, :, n * LANES : (n + 1) * LANES].reshape(2 * ROWS, LANES)
            x_col[n, rows, :] = (part * b_full[n : n + 1, :]).astype(BF16)

    loop(groups, first_operand)

    here = pl.ds(pl.multiple_of(col.me * LANES, LANES), LANES)
    mine = sbuf[:, :, here].astype(F32).reshape(sources, LANES)
    src_col[...] = mine
    src_col_sent[...] = mine.astype(BF16)
    for n, ref in enumerate((b_full, g_in, s_in, s_ahead)):
        vec_sent[n : n + 1, :] = ref[pl.ds(col.me, 1), :]
    vec_sent[4:8, :] = jnp.zeros((4, LANES), F32)
    src_turn = remote(src_col_sent, src_mom, turn_send.at[0], turn_recv.at[0], turned)
    vec_turn = remote(vec_sent, vec_mom, turn_send.at[1], turn_recv.at[1], turned)
    dv_turn = remote(dv_sent, dvbuf.at[mom.me], turn_send.at[2], turn_recv.at[2], turned)

    @pl.when(off_diagonal)
    def _():
        src_turn.start()
        vec_turn.start()

    def product(x, w, d):
        lhs = jnp.concatenate([x[n] for n in range(size)], axis=1)
        cols = pl.ds(pl.multiple_of(d * panel, panel), panel)
        return jnp.dot(lhs, w[:, cols], preferred_element_type=F32)

    def summed(a, x, w):
        def pair_copy(k):
            return remote(
                give.at[k], taken.at[a.which, k], rp_send.at[k], rp_recv.at[a.which, k], a.at(a.pair)
            )

        def mate_copy(k):
            t = a.order(k)
            return remote(
                hand.at[k],
                landed.at[a.which, t],
                rg_send.at[k],
                rg_recv.at[a.which, t],
                a.at(a.mate(t)),
            )

        first = a.parity == 0

        def multiply(k):
            both = product(x, w, (a.group + a.order(k)) % groups)
            low, high = both[:, :LANES], both[:, LANES:]
            keep[k] = jnp.where(first, low, high)
            give[k] = jnp.where(first, high, low).astype(BF16)
            pair_copy(k).start()

        loop(groups, multiply)

        def hand_on(k):
            pair_copy(k).wait_recv()
            hand[k] = (keep[k] + taken[a.which, k].astype(F32)).astype(BF16)
            mate_copy(k).start()

        loop(groups - 1, hand_on)
        pair_copy(groups - 1).wait_recv()
        total = keep[groups - 1] + taken[a.which, groups - 1].astype(F32)

        def add(k, total):
            mate_copy(k).wait_recv()
            return total + landed[a.which, a.order(k)].astype(F32)

        total = lax.fori_loop(0, groups - 1, add, total)

        def sent():
            loop(groups, lambda k: pair_copy(k).wait_send())
            loop(groups - 1, lambda k: mate_copy(k).wait_send())

        return total, sent

    mom_gather = Gather(mom, x_mom, x_mom.at[mom.me], sems_of(ag_sems, 0))
    col_gather = Gather(col, x_col, x_col.at[col.me], sems_of(ag_sems, 1))
    dv_gather = Gather(col, dvbuf, dvbuf.at[col.me], sems_of(dv_sems, 0))

    total, sent = summed(mom, x_col, v_mat)

    @pl.when(off_diagonal)
    def _():
        src_turn.wait()
        vec_turn.wait()

    @pl.when(jnp.logical_not(off_diagonal))
    def _():
        src_mom[...] = src_col_sent[...]
        vec_mom[...] = vec_sent[...]

    def mom_state(bubble, total):
        state = bubble * (src_mom[...].astype(F32) + total)
        x_mom[mom.me] = state.astype(BF16)
        return state

    def col_state(bubble, total):
        x_col[col.me] = (bubble * (src_col[...] + total)).astype(BF16)

    mom_state(vec_mom[0:1, :], total)
    mom_gather.start()
    sent()
    mom_gather.forward_all()
    mom_gather.finish()

    total, sent = summed(col, x_mom, v_turned)
    col_state(vec_sent[0:1, :], total)
    col_gather.start()
    sent()
    col_gather.forward_all()
    col_gather.finish()
    weight_gather.finish()

    total, sent = summed(mom, x_col, v_mat)
    ladder_first = mom_state(vec_mom[0:1, :], total)
    mom_gather.start()
    weights = wbuf[...].reshape(sources, LANES)
    self_energy = jnp.sum(weights * ladder_first, axis=0, keepdims=True)
    green = vec_mom[1:2, :]
    dressed = green + green * green * self_energy
    dre_sent[...] = jnp.broadcast_to(dressed, (ROWS, LANES))
    to_next = remote(dre_sent, dre_behind, behind_send, behind_recv, col.at((col.me + ahead) % size))
    to_next.start()
    sent()
    mom_gather.forward_all()
    to_next.wait()
    bubble_mom = -0.5 * (dressed * vec_mom[3:4, :] + vec_mom[2:3, :] * dre_behind[0:1, :])
    dv_sent[0:1, :] = dressed
    dv_sent[1:2, :] = bubble_mom
    dv_sent[2:8, :] = jnp.zeros((6, LANES), F32)

    @pl.when(off_diagonal)
    def _():
        dv_turn.start()

    mom_gather.finish()

    total, sent = summed(col, x_mom, v_turned)

    @pl.when(off_diagonal)
    def _():
        dv_turn.wait()

    @pl.when(jnp.logical_not(off_diagonal))
    def _():
        dvbuf[col.me] = dv_sent[...]

    col_state(dvbuf[col.me, 1:2, :], total)
    col_gather.start()
    dv_gather.start()
    sent()
    col_gather.forward_all()
    dv_gather.forward_all()
    col_gather.finish()

    total, sent = summed(mom, x_col, v_mat)
    mom_state(dv_sent[1:2, :], total)
    mom_gather.start()
    sent()
    mom_gather.forward_all()
    dv_gather.finish()
    mom_gather.finish()

    def last_product(d):
        both = product(x_mom, v_turned, d)
        cols = pl.ds(pl.multiple_of(d * panel, panel), panel)
        wide = both.reshape(size, ROWS, panel)
        fin_wide[:, :, cols] = wide
        fin[:, :, cols] = wide.astype(BF16)

    loop(groups, last_product)

    def fin_pair(k):
        there = col.mate(col.order(k)) + 1 - 2 * col.parity
        return remote(
            fin.at[there], fin_taken.at[k], rp_send.at[k], rp_recv.at[2, k], col.at(col.pair)
        )

    def fin_mate(k):
        t = col.order(k)
        return remote(
            fin_hand.at[k], fin_landed.at[t], rg_send.at[k], rg_recv.at[2, t], col.at(col.mate(t))
        )

    loop(groups, lambda k: fin_pair(k).start())

    def fin_sum(k):
        fin_pair(k).wait_recv()
        return fin_wide[col.mate(col.order(k))] + fin_taken[k].astype(F32)

    def fin_on(k):
        fin_hand[k] = fin_sum(k).astype(BF16)
        fin_mate(k).start()

    loop(groups - 1, fin_on)
    own[...] = fin_sum(groups - 1) + src[...].astype(F32)

    for n in range(size):
        dre_out[n : n + 1, :] = dvbuf[n, 0:1, :]

    def fin_add(k):
        fin_mate(k).wait_recv()
        own[...] += fin_landed[col.order(k)].astype(F32)

    loop(groups - 1, fin_add)
    for n in range(size):
        cols = slice(n * LANES, (n + 1) * LANES)
        lad_out[:, cols] = dvbuf[n, 1:2, :] * own[:, cols]

    loop(groups, lambda k: fin_pair(k).wait_send())
    loop(groups - 1, lambda k: fin_mate(k).wait_send())


def ladder_call(size, ahead):
    groups = size // 2
    sources = size * ROWS
    block = size * LANES
    slab = (sources, LANES)
    vmem = pl.BlockSpec(memory_space=pltpu.VMEM)
    dma = pltpu.SemaphoreType.DMA
    scratch = [
        pltpu.VMEM((block, block), BF16),
        pltpu.VMEM((block, block), BF16),
        pltpu.VMEM((size, *slab), BF16),
        pltpu.VMEM((size, *slab), BF16),
        pltpu.VMEM((size, ROWS, block), BF16),
        pltpu.VMEM((size, ROWS, LANES), F32),
        pltpu.VMEM((size, ROWS, LANES), F32),
        pltpu.VMEM((groups, *slab), F32),
        pltpu.VMEM((groups, *slab), BF16),
        pltpu.VMEM((2, groups, *slab), BF16),
        pltpu.VMEM((groups, *slab), BF16),
        pltpu.VMEM((2, groups, *slab), BF16),
        pltpu.VMEM((ROWS, block), F32),
        pltpu.VMEM((size, ROWS, block), F32),
        pltpu.VMEM((size, ROWS, block), BF16),
        pltpu.VMEM((groups, ROWS, block), BF16),
        pltpu.VMEM((groups, ROWS, block), BF16),
        pltpu.VMEM((groups, ROWS, block), BF16),
        pltpu.VMEM((size, LANES), F32),
        pltpu.VMEM((size, LANES), F32),
        pltpu.VMEM((size, LANES), F32),
        pltpu.VMEM(slab, F32),
        pltpu.VMEM(slab, BF16),
        pltpu.VMEM(slab, BF16),
        pltpu.VMEM((ROWS, LANES), F32),
        pltpu.VMEM((ROWS, LANES), F32),
        pltpu.VMEM((ROWS, LANES), F32),
        pltpu.VMEM((ROWS, LANES), F32),
        pltpu.VMEM((ROWS, LANES), F32),
        dma((groups,)),
        dma((2,)),
        dma((2,)),
        dma((3,)),
        dma((3,)),
        dma,
        dma,
        dma((2, 4, groups)),
        dma((1, 4, groups)),
        dma((1, 4, groups)),
        dma((groups,)),
        dma((3, groups)),
        dma((groups,)),
        dma((3, groups)),
    ]
    return pl.pallas_call(
        functools.partial(kernel, size, ahead),
        out_shape=(
            jax.ShapeDtypeStruct((ROWS, block), F32),
            jax.ShapeDtypeStruct((size, LANES), F32),
        ),
        in_specs=[pl.BlockSpec(memory_space=pl.ANY)] + [vmem] * 4,
        out_specs=(vmem, vmem),
        scratch_shapes=scratch,
        compiler_params=pltpu.CompilerParams(
            collective_id=0, has_side_effects=True, vmem_limit_bytes=48 * 1024 * 1024
        ),
        name="ladder",
    )


def body(ahead, vertex, sources, green_fn, green_shifted, leg_weights):
    size = lax.axis_size("mom")
    in_lanes = (size, LANES)
    ladder, dressed = ladder_call(size, ahead)(
        vertex,
        sources,
        green_fn.reshape(in_lanes),
        green_shifted.reshape(in_lanes),
        jnp.broadcast_to(leg_weights[:, None], (ROWS, LANES)),
    )
    return ladder, dressed.reshape(-1)


def solution(mesh):
    in_specs = (P("mom", "col"), P("col", "mom"), P("mom"), P("mom"), P("col"))
    out_specs = (P("col", "mom"), P("mom"))
    step = functools.partial(body, mesh.shape["mom"] // 4)
    return jax.shard_map(step, mesh=mesh, in_specs=in_specs, out_specs=out_specs, check_vma=False)
```

```python
import functools

import jax
import jax.numpy as jnp
from jax import lax
from jax.experimental import pallas as pl
from jax.experimental.pallas import tpu as pltpu
from jax.sharding import PartitionSpec as P

MESH = pl.DeviceIdType.MESH
LANES = 128
ROWS = 8
F32 = jnp.float32
BF16 = jnp.bfloat16


class Axis:
    def __init__(self, name, which, size):
        self.name = name
        self.which = which
        self.size = size
        self.groups = size // 2
        self.me = lax.axis_index(name)
        self.parity = self.me % 2
        self.group = self.me // 2
        self.pair = self.me + 1 - 2 * self.parity

    def at(self, index):
        return {self.name: index}

    def mate(self, steps):
        return 2 * ((self.group + steps) % self.groups) + self.parity

    def order(self, k):
        sign = 2 * (k % 2) - 1
        return (self.groups // 2 + sign * ((k + 1) // 2) + self.groups) % self.groups


def remote(src, dst, send, recv, device):
    return pltpu.make_async_remote_copy(
        src_ref=src,
        dst_ref=dst,
        send_sem=send,
        recv_sem=recv,
        device_id=device,
        device_id_type=MESH,
    )


def loop(count, step):
    def run(k, carry):
        step(k)
        return carry

    lax.fori_loop(0, count, run, 0)


class Gather:
    def __init__(self, axis, buf, sems, near):
        self.axis, self.buf, self.near = axis, buf, near
        self.mate_send, self.mate_recv, self.pair_send, self.pair_recv = sems

    def order(self, k):
        a = self.axis
        return a.order(a.groups - 2 - k) if self.near else a.order(k)

    def mate_copy(self, t):
        a = self.axis
        own = self.buf.at[a.me]
        return remote(own, own, self.mate_send.at[t], self.mate_recv.at[t], a.at(a.mate(t)))

    def pair_copy(self, t):
        a = self.axis
        block = self.buf.at[a.mate(a.groups - t)]
        return remote(block, block, self.pair_send.at[t], self.pair_recv.at[t], a.at(a.pair))

    def start(self):
        self.pair_copy(0).start()
        loop(self.axis.groups - 1, lambda k: self.mate_copy(self.order(k)).start())

    def forward(self, k):
        t = self.order(k)
        self.mate_copy(t).wait_recv()
        self.pair_copy(t).start()

    def forward_all(self):
        loop(self.axis.groups - 1, self.forward)

    def finish(self, use=None):
        a = self.axis

        def ended(t):
            self.pair_copy(t).wait_recv()
            if use is not None:
                use((a.group - t + a.groups) % a.groups)

        ended(0)
        loop(a.groups - 1, lambda k: ended(self.order(k)))

    def drain(self):
        loop(self.axis.groups, lambda k: self.pair_copy(k).wait_send())
        loop(self.axis.groups - 1, lambda k: self.mate_copy(k + 1).wait_send())


def kernel(
    size,
    ahead,
    v_hbm,
    src_hbm,
    g_hbm,
    s_hbm,
    w_hbm,
    lad_out,
    dre_out,
    v_mat,
    v_turned,
    x_mom,
    x_col,
    sbuf,
    wbuf,
    dvbuf,
    keep,
    give,
    taken,
    hand,
    landed,
    own,
    fin_wide,
    fin,
    fin_taken,
    fin_hand,
    fin_landed,
    b_full,
    s_ahead,
    g_behind,
    src_col,
    src_col_sent,
    src_mom,
    vec_sent,
    vec_mom,
    dre_sent,
    dre_behind,
    dv_sent,
    g_in,
    s_in,
    w_in,
    in_sem,
    v_sem,
    shift_send,
    shift_recv,
    turn_send,
    turn_recv,
    behind_send,
    behind_recv,
    ag_sems,
    w_sems,
    dv_sems,
    rp_send,
    rp_recv,
    rg_send,
    rg_recv,
):
    mom = Axis("mom", 0, size)
    col = Axis("col", 1, size)
    groups = size // 2
    sources = size * ROWS
    block = size * LANES
    panel = 2 * LANES

    def v_copy(k):
        rows = pl.ds(pl.multiple_of(k * panel, panel), panel)
        return pltpu.make_async_copy(v_hbm.at[rows], v_mat.at[rows], v_sem.at[k])

    inputs = (
        pltpu.make_async_copy(src_hbm, sbuf.at[col.me], in_sem.at[0]),
        pltpu.make_async_copy(s_hbm, s_in, in_sem.at[1]),
        pltpu.make_async_copy(g_hbm, g_in, in_sem.at[2]),
        pltpu.make_async_copy(w_hbm, w_in, in_sem.at[3]),
    )
    for copy in inputs:
        copy.start()

    barrier = pltpu.get_barrier_semaphore()
    for a in (mom, col):

        def greet(k, a=a):
            other = (a.me + k + 1) % size
            pl.semaphore_signal(barrier, inc=1, device_id=a.at(other), device_id_type=MESH)

        loop(size - 1, greet)
    turned = {"mom": col.me, "col": mom.me}
    off_diagonal = mom.me != col.me

    loop(groups, lambda k: v_copy(k).start())
    for copy in inputs:
        copy.wait()
    row = lax.broadcasted_iota(jnp.int32, (ROWS, LANES), 0)
    weight_rows = jnp.zeros((ROWS, LANES), F32)
    for n in range(ROWS):
        weight_rows = jnp.where(row == n, w_in[n], weight_rows)
    wbuf[col.me] = weight_rows
    pl.semaphore_wait(barrier, 2 * (size - 1))

    def sems_of(ref, which):
        return tuple(ref.at[which, n] for n in range(4))

    to_behind = remote(
        s_in, s_ahead, shift_send.at[0], shift_recv.at[0], mom.at((mom.me + size - ahead) % size)
    )
    to_ahead = remote(g_in, g_behind, shift_send.at[1], shift_recv.at[1], mom.at((mom.me + ahead) % size))
    source_gather = Gather(col, sbuf, sems_of(ag_sems, 1), near=True)
    source_gather.start()
    to_behind.start()
    to_ahead.start()
    weight_gather = Gather(col, wbuf, sems_of(w_sems, 0), near=True)
    weight_gather.start()

    def turn_panel(k):
        rows = pl.ds(pl.multiple_of(k * panel, panel), panel)
        for n in range(groups):
            cols = slice(n * panel, (n + 1) * panel)
            v_turned[cols, rows] = v_mat[rows, cols].T

    early = min(3, groups - 1)
    loop(groups, lambda k: v_copy(k).wait())
    loop(early, turn_panel)
    source_gather.forward_all()
    weight_gather.forward_all()

    to_behind.wait()
    to_ahead.wait()
    b_full[...] = -0.5 * (g_in[...] * s_ahead[...] + s_in[...] * g_behind[...])

    def first_operand(k):
        two = sbuf[pl.ds(2 * k, 2)].astype(F32)
        rows = pl.ds(pl.multiple_of(2 * ROWS * k, 2 * ROWS), 2 * ROWS)
        for n in range(size):
            part = two[:, :, n * LANES : (n + 1) * LANES].reshape(2 * ROWS, LANES)
            x_col[n, rows, :] = (part * b_full[n : n + 1, :]).astype(BF16)

    source_gather.finish(first_operand)
    source_gather.drain()

    here = pl.ds(pl.multiple_of(col.me * LANES, LANES), LANES)
    mine = sbuf[:, :, here].astype(F32).reshape(sources, LANES)
    src_col[...] = mine
    src_col_sent[...] = mine.astype(BF16)
    for n, ref in enumerate((b_full, g_in, s_in, s_ahead)):
        vec_sent[n : n + 1, :] = ref[pl.ds(col.me, 1), :]
    vec_sent[4:8, :] = jnp.zeros((4, LANES), F32)
    src_turn = remote(src_col_sent, src_mom, turn_send.at[0], turn_recv.at[0], turned)
    vec_turn = remote(vec_sent, vec_mom, turn_send.at[1], turn_recv.at[1], turned)
    dv_turn = remote(dv_sent, dvbuf.at[mom.me], turn_send.at[2], turn_recv.at[2], turned)

    @pl.when(off_diagonal)
    def _():
        src_turn.start()
        vec_turn.start()

    def product(x, w, d):
        lhs = jnp.concatenate([x[n] for n in range(size)], axis=1)
        cols = pl.ds(pl.multiple_of(d * panel, panel), panel)
        return jnp.dot(lhs, w[:, cols], preferred_element_type=F32)

    def summed(a, x, w, lag, meanwhile=None):
        lag = min(lag, groups - 1)

        def pair_copy(k):
            return remote(
                give.at[k], taken.at[a.which, k], rp_send.at[0, k], rp_recv.at[a.which, k], a.at(a.pair)
            )

        def mate_copy(k):
            t = a.order(k)
            return remote(
                hand.at[k],
                landed.at[a.which, t],
                rg_send.at[0, k],
                rg_recv.at[a.which, t],
                a.at(a.mate(t)),
            )

        first = a.parity == 0

        def multiply(k):
            both = product(x, w, (a.group + a.order(k)) % groups)
            low, high = both[:, :LANES], both[:, LANES:]
            keep[k] = jnp.where(first, low, high)
            give[k] = jnp.where(first, high, low).astype(BF16)
            pair_copy(k).start()

        def hand_on(k):
            pair_copy(k).wait_recv()
            hand[k] = (keep[k] + taken[a.which, k].astype(F32)).astype(BF16)
            mate_copy(k).start()

        def both_stages(k):
            multiply(k + lag)
            hand_on(k)

        loop(lag, multiply)
        loop(groups - lag, both_stages)
        loop(lag - 1, lambda k: hand_on(k + groups - lag))
        if meanwhile is not None:
            meanwhile()
        pair_copy(groups - 1).wait_recv()
        total = keep[groups - 1] + taken[a.which, groups - 1].astype(F32)

        def add(k, total):
            mate_copy(k).wait_recv()
            return total + landed[a.which, a.order(k)].astype(F32)

        total = lax.fori_loop(0, groups - 1, add, total)

        def sent():
            loop(groups, lambda k: pair_copy(k).wait_send())
            loop(groups - 1, lambda k: mate_copy(k).wait_send())

        return total, sent

    mom_gather = Gather(mom, x_mom, sems_of(ag_sems, 0), near=False)
    col_gather = Gather(col, x_col, sems_of(ag_sems, 1), near=True)
    dv_gather = Gather(col, dvbuf, sems_of(dv_sems, 0), near=True)

    total, sent = summed(
        mom, x_col, v_mat, 3, lambda: loop(groups - early, lambda k: turn_panel(k + early))
    )

    @pl.when(off_diagonal)
    def _():
        src_turn.wait()
        vec_turn.wait()

    @pl.when(jnp.logical_not(off_diagonal))
    def _():
        src_mom[...] = src_col_sent[...]
        vec_mom[...] = vec_sent[...]

    def mom_state(bubble, total):
        state = bubble * (src_mom[...].astype(F32) + total)
        x_mom[mom.me] = state.astype(BF16)
        return state

    def col_state(bubble, total):
        x_col[col.me] = (bubble * (src_col[...] + total)).astype(BF16)

    mom_state(vec_mom[0:1, :], total)
    mom_gather.start()
    sent()
    mom_gather.forward_all()
    mom_gather.finish()

    total, sent = summed(col, x_mom, v_turned, 6)
    mom_gather.drain()
    col_state(vec_sent[0:1, :], total)
    col_gather.start()
    sent()
    col_gather.forward_all()
    col_gather.finish()
    weight_gather.finish()
    weight_gather.drain()

    total, sent = summed(mom, x_col, v_mat, 3)
    col_gather.drain()
    ladder_first = mom_state(vec_mom[0:1, :], total)
    mom_gather.start()
    weights = wbuf[...].reshape(sources, LANES)
    self_energy = jnp.sum(weights * ladder_first, axis=0, keepdims=True)
    green = vec_mom[1:2, :]
    dressed = green + green * green * self_energy
    dre_sent[...] = jnp.broadcast_to(dressed, (ROWS, LANES))
    to_next = remote(dre_sent, dre_behind, behind_send, behind_recv, col.at((col.me + ahead) % size))
    to_next.start()
    sent()
    mom_gather.forward_all()
    to_next.wait()
    bubble_mom = -0.5 * (dressed * vec_mom[3:4, :] + vec_mom[2:3, :] * dre_behind[0:1, :])
    dv_sent[0:1, :] = dressed
    dv_sent[1:2, :] = bubble_mom
    dv_sent[2:8, :] = jnp.zeros((6, LANES), F32)

    @pl.when(off_diagonal)
    def _():
        dv_turn.start()

    mom_gather.finish()

    total, sent = summed(col, x_mom, v_turned, 6)
    mom_gather.drain()

    @pl.when(off_diagonal)
    def _():
        dv_turn.wait()

    @pl.when(jnp.logical_not(off_diagonal))
    def _():
        dvbuf[col.me] = dv_sent[...]

    col_state(dvbuf[col.me, 1:2, :], total)
    col_gather.start()
    dv_gather.start()
    sent()
    col_gather.forward_all()
    dv_gather.forward_all()
    col_gather.finish()

    total, sent = summed(mom, x_col, v_mat, 3)
    col_gather.drain()
    mom_state(dv_sent[1:2, :], total)
    mom_gather.start()
    sent()
    mom_gather.forward_all()
    dv_gather.finish()
    dv_gather.drain()
    mom_gather.finish()

    half = block // 2

    def lanes(h):
        return pl.ds(pl.multiple_of(h * half, half), half)

    def last_product(d):
        both = product(x_mom, v_turned, d)
        cols = pl.ds(pl.multiple_of(d * panel, panel), panel)
        wide = both.reshape(size, ROWS, panel)
        fin_wide[:, :, cols] = wide
        fin[:, :, cols] = wide.astype(BF16)

    def fin_pair(k, h):
        there = col.mate(col.order(k)) + 1 - 2 * col.parity
        return remote(
            fin.at[there, :, lanes(h)],
            fin_taken.at[k, :, lanes(h)],
            rp_send.at[h, k],
            rp_recv.at[2 + h, k],
            col.at(col.pair),
        )

    def fin_mate(k, h):
        t = col.order(k)
        return remote(
            fin_hand.at[k, :, lanes(h)],
            fin_landed.at[t, :, lanes(h)],
            rg_send.at[h, k],
            rg_recv.at[2 + h, t],
            col.at(col.mate(t)),
        )

    def fin_sum(k, h):
        fin_pair(k, h).wait_recv()
        kept = fin_wide[col.mate(col.order(k)), :, lanes(h)]
        return kept + fin_taken[k, :, lanes(h)].astype(F32)

    def fin_on(k, h):
        fin_hand[k, :, lanes(h)] = fin_sum(k, h).astype(BF16)
        fin_mate(k, h).start()

    def fin_half(h):
        loop(groups // 2, lambda k: last_product(h * (groups // 2) + k))
        loop(groups, lambda k: fin_pair(k, h).start())

    loop(2, fin_half)
    mom_gather.drain()
    for h in range(2):
        loop(groups - 1, lambda k, h=h: fin_on(k, h))
        own[:, lanes(h)] = fin_sum(groups - 1, h) + sbuf[col.me, :, lanes(h)].astype(F32)

    for n in range(size):
        dre_out[n : n + 1, :] = dvbuf[n, 0:1, :]

    def fin_add(k, h):
        fin_mate(k, h).wait_recv()
        own[:, lanes(h)] += fin_landed[col.order(k), :, lanes(h)].astype(F32)

    for h in range(2):
        loop(groups - 1, lambda k, h=h: fin_add(k, h))
    for n in range(size):
        cols = slice(n * LANES, (n + 1) * LANES)
        lad_out[:, cols] = dvbuf[n, 1:2, :] * own[:, cols]

    for h in range(2):
        loop(groups, lambda k, h=h: fin_pair(k, h).wait_send())
        loop(groups - 1, lambda k, h=h: fin_mate(k, h).wait_send())


def ladder_call(size, ahead):
    groups = size // 2
    sources = size * ROWS
    block = size * LANES
    slab = (sources, LANES)
    vmem = pl.BlockSpec(memory_space=pltpu.VMEM)
    dma = pltpu.SemaphoreType.DMA
    scratch = [
        pltpu.VMEM((block, block), BF16),
        pltpu.VMEM((block, block), BF16),
        pltpu.VMEM((size, *slab), BF16),
        pltpu.VMEM((size, *slab), BF16),
        pltpu.VMEM((size, ROWS, block), BF16),
        pltpu.VMEM((size, ROWS, LANES), F32),
        pltpu.VMEM((size, ROWS, LANES), F32),
        pltpu.VMEM((groups, *slab), F32),
        pltpu.VMEM((groups, *slab), BF16),
        pltpu.VMEM((2, groups, *slab), BF16),
        pltpu.VMEM((groups, *slab), BF16),
        pltpu.VMEM((2, groups, *slab), BF16),
        pltpu.VMEM((ROWS, block), F32),
        pltpu.VMEM((size, ROWS, block), F32),
        pltpu.VMEM((size, ROWS, block), BF16),
        pltpu.VMEM((groups, ROWS, block), BF16),
        pltpu.VMEM((groups, ROWS, block), BF16),
        pltpu.VMEM((groups, ROWS, block), BF16),
        pltpu.VMEM((size, LANES), F32),
        pltpu.VMEM((size, LANES), F32),
        pltpu.VMEM((size, LANES), F32),
        pltpu.VMEM(slab, F32),
        pltpu.VMEM(slab, BF16),
        pltpu.VMEM(slab, BF16),
        pltpu.VMEM((ROWS, LANES), F32),
        pltpu.VMEM((ROWS, LANES), F32),
        pltpu.VMEM((ROWS, LANES), F32),
        pltpu.VMEM((ROWS, LANES), F32),
        pltpu.VMEM((ROWS, LANES), F32),
        pltpu.VMEM((size, LANES), F32),
        pltpu.VMEM((size, LANES), F32),
        pltpu.SMEM((ROWS,), F32),
        dma((4,)),
        dma((groups,)),
        dma((2,)),
        dma((2,)),
        dma((3,)),
        dma((3,)),
        dma,
        dma,
        dma((2, 4, groups)),
        dma((1, 4, groups)),
        dma((1, 4, groups)),
        dma((2, groups)),
        dma((4, groups)),
        dma((2, groups)),
        dma((4, groups)),
    ]
    return pl.pallas_call(
        functools.partial(kernel, size, ahead),
        out_shape=(
            jax.ShapeDtypeStruct((ROWS, block), F32),
            jax.ShapeDtypeStruct((size, LANES), F32),
        ),
        in_specs=[pl.BlockSpec(memory_space=pltpu.HBM)] * 5,
        out_specs=(vmem, vmem),
        scratch_shapes=scratch,
        compiler_params=pltpu.CompilerParams(
            collective_id=0, has_side_effects=True, vmem_limit_bytes=48 * 1024 * 1024
        ),
        name="ladder",
    )


def body(ahead, vertex, sources, green_fn, green_shifted, leg_weights):
    size = lax.axis_size("mom")
    in_lanes = (size, LANES)
    in_hbm = [
        pltpu.with_memory_space_constraint(x, pltpu.HBM)
        for x in (vertex, sources, green_fn.reshape(in_lanes), green_shifted.reshape(in_lanes), leg_weights)
    ]
    ladder, dressed = ladder_call(size, ahead)(*in_hbm)
    return ladder, dressed.reshape(-1)


def solution(mesh):
    in_specs = (P("mom", "col"), P("col", "mom"), P("mom"), P("mom"), P("col"))
    out_specs = (P("col", "mom"), P("mom"))
    step = functools.partial(body, mesh.shape["mom"] // 4)
    return jax.shard_map(step, mesh=mesh, in_specs=in_specs, out_specs=out_specs, check_vma=False)
```

```python
import functools

import jax
import jax.numpy as jnp
from jax import lax
from jax.experimental import pallas as pl
from jax.experimental.pallas import tpu as pltpu
from jax.sharding import PartitionSpec as P

MESH = pl.DeviceIdType.MESH
LANES = 128
ROWS = 8
F32 = jnp.float32
BF16 = jnp.bfloat16


class Axis:
    def __init__(self, name, which, size):
        self.name = name
        self.which = which
        self.size = size
        self.groups = size // 2
        self.me = lax.axis_index(name)
        self.parity = self.me % 2
        self.group = self.me // 2
        self.pair = self.me + 1 - 2 * self.parity

    def at(self, index):
        return {self.name: index}

    def mate(self, steps):
        return 2 * ((self.group + steps) % self.groups) + self.parity

    def order(self, k):
        if self.which == 0 and self.groups == 8:
            late, rest = k // 4, k % 4
            sign = (1 - 2 * (rest % 2)) * (1 - 2 * late)
            return (5 - late + sign * 2 * ((rest + 1) // 2) + 8) % 8
        sign = 2 * (k % 2) - 1
        return (self.groups // 2 + sign * ((k + 1) // 2) + self.groups) % self.groups


def remote(src, dst, send, recv, device):
    return pltpu.make_async_remote_copy(
        src_ref=src,
        dst_ref=dst,
        send_sem=send,
        recv_sem=recv,
        device_id=device,
        device_id_type=MESH,
    )


def loop(count, step):
    def run(k, carry):
        step(k)
        return carry

    lax.fori_loop(0, count, run, 0)


class Gather:
    def __init__(self, axis, buf, sems, near):
        self.axis, self.buf, self.near = axis, buf, near
        self.mate_send, self.mate_recv, self.pair_send, self.pair_recv = sems

    def order(self, k):
        a = self.axis
        return a.order(a.groups - 2 - k) if self.near else a.order(k)

    def mate_copy(self, t):
        a = self.axis
        own = self.buf.at[a.me]
        return remote(own, own, self.mate_send.at[t], self.mate_recv.at[t], a.at(a.mate(t)))

    def pair_copy(self, t):
        a = self.axis
        block = self.buf.at[a.mate(a.groups - t)]
        return remote(block, block, self.pair_send.at[t], self.pair_recv.at[t], a.at(a.pair))

    def start(self):
        self.pair_copy(0).start()
        loop(self.axis.groups - 1, lambda k: self.mate_copy(self.order(k)).start())

    def forward(self, k):
        t = self.order(k)
        self.mate_copy(t).wait_recv()
        self.pair_copy(t).start()

    def forward_all(self):
        loop(self.axis.groups - 1, self.forward)

    def finish(self, use=None):
        a = self.axis

        def ended(t):
            self.pair_copy(t).wait_recv()
            if use is not None:
                use((a.group - t + a.groups) % a.groups)

        ended(0)
        loop(a.groups - 1, lambda k: ended(self.order(k)))

    def drain(self):
        loop(self.axis.groups, lambda k: self.pair_copy(k).wait_send())
        loop(self.axis.groups - 1, lambda k: self.mate_copy(k + 1).wait_send())


def kernel(
    size,
    ahead,
    v_hbm,
    src_hbm,
    g_hbm,
    s_hbm,
    w_hbm,
    lad_out,
    dre_out,
    v_mat,
    v_turned,
    x_mom,
    x_col,
    sbuf,
    wbuf,
    dvbuf,
    keep,
    give,
    taken,
    hand,
    landed,
    own,
    fin_wide,
    fin,
    fin_taken,
    fin_hand,
    fin_landed,
    b_full,
    s_ahead,
    g_behind,
    src_col,
    src_col_sent,
    src_mom,
    vec_sent,
    vec_mom,
    dre_sent,
    dre_behind,
    dv_sent,
    g_in,
    s_in,
    w_in,
    in_sem,
    v_sem,
    shift_send,
    shift_recv,
    turn_send,
    turn_recv,
    behind_send,
    behind_recv,
    ag_sems,
    w_sems,
    dv_sems,
    rp_send,
    rp_recv,
    rg_send,
    rg_recv,
):
    mom = Axis("mom", 0, size)
    col = Axis("col", 1, size)
    groups = size // 2
    sources = size * ROWS
    block = size * LANES
    panel = 2 * LANES

    def v_copy(k):
        rows = pl.ds(pl.multiple_of(k * panel, panel), panel)
        return pltpu.make_async_copy(v_hbm.at[rows], v_mat.at[rows], v_sem.at[k])

    inputs = (
        pltpu.make_async_copy(src_hbm, sbuf.at[col.me], in_sem.at[0]),
        pltpu.make_async_copy(s_hbm, s_in, in_sem.at[1]),
        pltpu.make_async_copy(g_hbm, g_in, in_sem.at[2]),
        pltpu.make_async_copy(w_hbm, w_in, in_sem.at[3]),
    )
    for copy in inputs:
        copy.start()

    barrier = pltpu.get_barrier_semaphore()
    for a in (mom, col):

        def greet(k, a=a):
            other = (a.me + k + 1) % size
            pl.semaphore_signal(barrier, inc=1, device_id=a.at(other), device_id_type=MESH)

        loop(size - 1, greet)
    turned = {"mom": col.me, "col": mom.me}
    off_diagonal = mom.me != col.me

    loop(groups, lambda k: v_copy(k).start())
    for copy in inputs:
        copy.wait()
    row = lax.broadcasted_iota(jnp.int32, (ROWS, LANES), 0)
    weight_rows = jnp.zeros((ROWS, LANES), F32)
    for n in range(ROWS):
        weight_rows = jnp.where(row == n, w_in[n], weight_rows)
    wbuf[col.me] = weight_rows
    pl.semaphore_wait(barrier, 2 * (size - 1))

    def sems_of(ref, which):
        return tuple(ref.at[which, n] for n in range(4))

    to_behind = remote(
        s_in, s_ahead, shift_send.at[0], shift_recv.at[0], mom.at((mom.me + size - ahead) % size)
    )
    to_ahead = remote(g_in, g_behind, shift_send.at[1], shift_recv.at[1], mom.at((mom.me + ahead) % size))
    source_gather = Gather(col, sbuf, sems_of(ag_sems, 1), near=True)
    source_gather.start()
    to_behind.start()
    to_ahead.start()
    weight_gather = Gather(col, wbuf, sems_of(w_sems, 0), near=True)
    weight_gather.start()

    def turn_panel(k):
        rows = pl.ds(pl.multiple_of(k * panel, panel), panel)
        for n in range(groups):
            cols = slice(n * panel, (n + 1) * panel)
            v_turned[cols, rows] = v_mat[rows, cols].T

    early = min(3, groups - 1)
    loop(groups, lambda k: v_copy(k).wait())
    loop(early, turn_panel)
    source_gather.forward_all()
    weight_gather.forward_all()

    to_behind.wait()
    to_ahead.wait()
    b_full[...] = -0.5 * (g_in[...] * s_ahead[...] + s_in[...] * g_behind[...])

    def first_operand(k):
        two = sbuf[pl.ds(2 * k, 2)].astype(F32)
        rows = pl.ds(pl.multiple_of(2 * ROWS * k, 2 * ROWS), 2 * ROWS)
        for n in range(size):
            part = two[:, :, n * LANES : (n + 1) * LANES].reshape(2 * ROWS, LANES)
            x_col[n, rows, :] = (part * b_full[n : n + 1, :]).astype(BF16)

    source_gather.finish(first_operand)
    source_gather.drain()

    here = pl.ds(pl.multiple_of(col.me * LANES, LANES), LANES)
    mine = sbuf[:, :, here].astype(F32).reshape(sources, LANES)
    src_col[...] = mine
    src_col_sent[...] = mine.astype(BF16)
    for n, ref in enumerate((b_full, g_in, s_in, s_ahead)):
        vec_sent[n : n + 1, :] = ref[pl.ds(col.me, 1), :]
    vec_sent[4:8, :] = jnp.zeros((4, LANES), F32)
    src_turn = remote(src_col_sent, src_mom, turn_send.at[0], turn_recv.at[0], turned)
    vec_turn = remote(vec_sent, vec_mom, turn_send.at[1], turn_recv.at[1], turned)
    dv_turn = remote(dv_sent, dvbuf.at[mom.me], turn_send.at[2], turn_recv.at[2], turned)

    @pl.when(off_diagonal)
    def _():
        src_turn.start()
        vec_turn.start()

    def product(x, w, d):
        lhs = jnp.concatenate([x[n] for n in range(size)], axis=1)
        cols = pl.ds(pl.multiple_of(d * panel, panel), panel)
        return jnp.dot(lhs, w[:, cols], preferred_element_type=F32)

    def summed(a, x, w, lag, meanwhile=None):
        lag = min(lag, groups - 1)

        def pair_copy(k):
            return remote(
                give.at[k], taken.at[a.which, k], rp_send.at[0, k], rp_recv.at[a.which, k], a.at(a.pair)
            )

        def mate_copy(k):
            t = a.order(k)
            return remote(
                hand.at[k],
                landed.at[a.which, t],
                rg_send.at[0, k],
                rg_recv.at[a.which, t],
                a.at(a.mate(t)),
            )

        first = a.parity == 0

        def multiply(k):
            both = product(x, w, (a.group + a.order(k)) % groups)
            low, high = both[:, :LANES], both[:, LANES:]
            keep[k] = jnp.where(first, low, high)
            give[k] = jnp.where(first, high, low).astype(BF16)
            pair_copy(k).start()

        def hand_on(k):
            pair_copy(k).wait_recv()
            hand[k] = (keep[k] + taken[a.which, k].astype(F32)).astype(BF16)
            mate_copy(k).start()

        def both_stages(k):
            multiply(k + lag)
            hand_on(k)

        loop(lag, multiply)
        loop(groups - lag, both_stages)
        loop(lag - 1, lambda k: hand_on(k + groups - lag))
        if meanwhile is not None:
            meanwhile()
        pair_copy(groups - 1).wait_recv()
        total = keep[groups - 1] + taken[a.which, groups - 1].astype(F32)

        def add(k, total):
            mate_copy(k).wait_recv()
            return total + landed[a.which, a.order(k)].astype(F32)

        total = lax.fori_loop(0, groups - 1, add, total)

        def sent():
            loop(groups, lambda k: pair_copy(k).wait_send())
            loop(groups - 1, lambda k: mate_copy(k).wait_send())

        return total, sent

    mom_gather = Gather(mom, x_mom, sems_of(ag_sems, 0), near=False)
    col_gather = Gather(col, x_col, sems_of(ag_sems, 1), near=True)
    dv_gather = Gather(col, dvbuf, sems_of(dv_sems, 0), near=True)

    total, sent = summed(
        mom, x_col, v_mat, 3, lambda: loop(groups - early, lambda k: turn_panel(k + early))
    )

    @pl.when(off_diagonal)
    def _():
        src_turn.wait()
        vec_turn.wait()

    @pl.when(jnp.logical_not(off_diagonal))
    def _():
        src_mom[...] = src_col_sent[...]
        vec_mom[...] = vec_sent[...]

    def mom_state(bubble, total):
        state = bubble * (src_mom[...].astype(F32) + total)
        x_mom[mom.me] = state.astype(BF16)
        return state

    def col_state(bubble, total):
        x_col[col.me] = (bubble * (src_col[...] + total)).astype(BF16)

    mom_state(vec_mom[0:1, :], total)
    mom_gather.start()
    sent()
    mom_gather.forward_all()
    mom_gather.finish()

    total, sent = summed(col, x_mom, v_turned, 6)
    mom_gather.drain()
    col_state(vec_sent[0:1, :], total)
    col_gather.start()
    sent()
    col_gather.forward_all()
    col_gather.finish()
    weight_gather.finish()
    weight_gather.drain()

    total, sent = summed(mom, x_col, v_mat, 3)
    col_gather.drain()
    ladder_first = mom_state(vec_mom[0:1, :], total)
    mom_gather.start()
    weights = wbuf[...].reshape(sources, LANES)
    self_energy = jnp.sum(weights * ladder_first, axis=0, keepdims=True)
    green = vec_mom[1:2, :]
    dressed = green + green * green * self_energy
    dre_sent[...] = jnp.broadcast_to(dressed, (ROWS, LANES))
    to_next = remote(dre_sent, dre_behind, behind_send, behind_recv, col.at((col.me + ahead) % size))
    to_next.start()
    sent()
    mom_gather.forward_all()
    to_next.wait()
    bubble_mom = -0.5 * (dressed * vec_mom[3:4, :] + vec_mom[2:3, :] * dre_behind[0:1, :])
    dv_sent[0:1, :] = dressed
    dv_sent[1:2, :] = bubble_mom
    dv_sent[2:8, :] = jnp.zeros((6, LANES), F32)

    @pl.when(off_diagonal)
    def _():
        dv_turn.start()

    mom_gather.finish()

    total, sent = summed(col, x_mom, v_turned, 6)
    mom_gather.drain()

    @pl.when(off_diagonal)
    def _():
        dv_turn.wait()

    @pl.when(jnp.logical_not(off_diagonal))
    def _():
        dvbuf[col.me] = dv_sent[...]

    col_state(dvbuf[col.me, 1:2, :], total)
    col_gather.start()
    dv_gather.start()
    sent()
    col_gather.forward_all()
    dv_gather.forward_all()
    col_gather.finish()

    total, sent = summed(mom, x_col, v_mat, 3)
    col_gather.drain()
    mom_state(dv_sent[1:2, :], total)
    mom_gather.start()
    sent()
    mom_gather.forward_all()
    dv_gather.finish()
    dv_gather.drain()
    mom_gather.finish()

    half = block // 2

    def lanes(h):
        return pl.ds(pl.multiple_of(h * half, half), half)

    def last_product(d):
        both = product(x_mom, v_turned, d)
        cols = pl.ds(pl.multiple_of(d * panel, panel), panel)
        wide = both.reshape(size, ROWS, panel)
        fin_wide[:, :, cols] = wide
        fin[:, :, cols] = wide.astype(BF16)

    def fin_pair(k, h):
        there = col.mate(col.order(k)) + 1 - 2 * col.parity
        return remote(
            fin.at[there, :, lanes(h)],
            fin_taken.at[k, :, lanes(h)],
            rp_send.at[h, k],
            rp_recv.at[2 + h, k],
            col.at(col.pair),
        )

    def fin_mate(k, h):
        t = col.order(k)
        return remote(
            fin_hand.at[k, :, lanes(h)],
            fin_landed.at[t, :, lanes(h)],
            rg_send.at[h, k],
            rg_recv.at[2 + h, t],
            col.at(col.mate(t)),
        )

    def fin_sum(k, h):
        fin_pair(k, h).wait_recv()
        kept = fin_wide[col.mate(col.order(k)), :, lanes(h)]
        return kept + fin_taken[k, :, lanes(h)].astype(F32)

    def fin_on(k, h):
        fin_hand[k, :, lanes(h)] = fin_sum(k, h).astype(BF16)
        fin_mate(k, h).start()

    def fin_half(h):
        loop(groups // 2, lambda k: last_product(h * (groups // 2) + k))
        loop(groups, lambda k: fin_pair(k, h).start())

    loop(2, fin_half)
    mom_gather.drain()
    for h in range(2):
        loop(groups - 1, lambda k, h=h: fin_on(k, h))
        own[:, lanes(h)] = fin_sum(groups - 1, h) + sbuf[col.me, :, lanes(h)].astype(F32)

    for n in range(size):
        dre_out[n : n + 1, :] = dvbuf[n, 0:1, :]

    def fin_add(k, h):
        fin_mate(k, h).wait_recv()
        own[:, lanes(h)] += fin_landed[col.order(k), :, lanes(h)].astype(F32)

    for h in range(2):
        loop(groups - 1, lambda k, h=h: fin_add(k, h))
    for n in range(size):
        cols = slice(n * LANES, (n + 1) * LANES)
        lad_out[:, cols] = dvbuf[n, 1:2, :] * own[:, cols]

    for h in range(2):
        loop(groups, lambda k, h=h: fin_pair(k, h).wait_send())
        loop(groups - 1, lambda k, h=h: fin_mate(k, h).wait_send())


def ladder_call(size, ahead):
    groups = size // 2
    sources = size * ROWS
    block = size * LANES
    slab = (sources, LANES)
    vmem = pl.BlockSpec(memory_space=pltpu.VMEM)
    dma = pltpu.SemaphoreType.DMA
    scratch = [
        pltpu.VMEM((block, block), BF16),
        pltpu.VMEM((block, block), BF16),
        pltpu.VMEM((size, *slab), BF16),
        pltpu.VMEM((size, *slab), BF16),
        pltpu.VMEM((size, ROWS, block), BF16),
        pltpu.VMEM((size, ROWS, LANES), F32),
        pltpu.VMEM((size, ROWS, LANES), F32),
        pltpu.VMEM((groups, *slab), F32),
        pltpu.VMEM((groups, *slab), BF16),
        pltpu.VMEM((2, groups, *slab), BF16),
        pltpu.VMEM((groups, *slab), BF16),
        pltpu.VMEM((2, groups, *slab), BF16),
        pltpu.VMEM((ROWS, block), F32),
        pltpu.VMEM((size, ROWS, block), F32),
        pltpu.VMEM((size, ROWS, block), BF16),
        pltpu.VMEM((groups, ROWS, block), BF16),
        pltpu.VMEM((groups, ROWS, block), BF16),
        pltpu.VMEM((groups, ROWS, block), BF16),
        pltpu.VMEM((size, LANES), F32),
        pltpu.VMEM((size, LANES), F32),
        pltpu.VMEM((size, LANES), F32),
        pltpu.VMEM(slab, F32),
        pltpu.VMEM(slab, BF16),
        pltpu.VMEM(slab, BF16),
        pltpu.VMEM((ROWS, LANES), F32),
        pltpu.VMEM((ROWS, LANES), F32),
        pltpu.VMEM((ROWS, LANES), F32),
        pltpu.VMEM((ROWS, LANES), F32),
        pltpu.VMEM((ROWS, LANES), F32),
        pltpu.VMEM((size, LANES), F32),
        pltpu.VMEM((size, LANES), F32),
        pltpu.SMEM((ROWS,), F32),
        dma((4,)),
        dma((groups,)),
        dma((2,)),
        dma((2,)),
        dma((3,)),
        dma((3,)),
        dma,
        dma,
        dma((2, 4, groups)),
        dma((1, 4, groups)),
        dma((1, 4, groups)),
        dma((2, groups)),
        dma((4, groups)),
        dma((2, groups)),
        dma((4, groups)),
    ]
    return pl.pallas_call(
        functools.partial(kernel, size, ahead),
        out_shape=(
            jax.ShapeDtypeStruct((ROWS, block), F32),
            jax.ShapeDtypeStruct((size, LANES), F32),
        ),
        in_specs=[pl.BlockSpec(memory_space=pltpu.HBM)] * 5,
        out_specs=(vmem, vmem),
        scratch_shapes=scratch,
        compiler_params=pltpu.CompilerParams(
            collective_id=0, has_side_effects=True, vmem_limit_bytes=48 * 1024 * 1024
        ),
        name="ladder",
    )


def body(ahead, vertex, sources, green_fn, green_shifted, leg_weights):
    size = lax.axis_size("mom")
    in_lanes = (size, LANES)
    in_hbm = [
        pltpu.with_memory_space_constraint(x, pltpu.HBM)
        for x in (vertex, sources, green_fn.reshape(in_lanes), green_shifted.reshape(in_lanes), leg_weights)
    ]
    ladder, dressed = ladder_call(size, ahead)(*in_hbm)
    return ladder, dressed.reshape(-1)


def solution(mesh):
    in_specs = (P("mom", "col"), P("col", "mom"), P("mom"), P("mom"), P("col"))
    out_specs = (P("col", "mom"), P("mom"))
    step = functools.partial(body, mesh.shape["mom"] // 4)
    return jax.shard_map(step, mesh=mesh, in_specs=in_specs, out_specs=out_specs, check_vma=False)
```
